768 devices in a mesh: dp: 12 (over z), tensor: 64 (over y, x, core).
Axes of the slice: x: 4, y: 8, z: 12, core: 2. Of those that a mesh axis runs over, the one named last changes fastest.
Arguments:
- gradients: bfloat16 [12, 192, 512, 512], P('dp', None, 'tensor'), may hold values from -240 to 240
- momentum: bfloat16 [12, 36, 512, 512], P('dp', None, 'tensor'), may hold values from -36 to 36
- owners: int32 [192], replicated, may hold values from 0 to 11, as said below
Outputs:
- updates: float32 [12, 36, 512, 512], P('dp', None, 'tensor')
The draws below stay inside these ranges and needn't reach their ends.
Inputs may be any that keep to these rules, and one draw needn't show every extreme that they name: `owners`: the blocks b with b // 16 == h give at most 3 blocks to any one owner, and exactly 3 to some owner, for every h; each owner holds at most 36 blocks, and some owner holds exactly 36.
All inputs are finite; a program needn't handle non-finite values.
Results may differ from the reference program's by a relative error of at most 0.018.
Values may be sent and summed in bfloat16 or wider, within the bound.
No kernel may reach another device: no remote copies, remote signals or barrier semaphores. Data moves between devices by JAX's collectives and lax.ppermute only.
A program may use at most 32 MiB of HBM per device.

```python
import math
import jax
import jax.numpy as jnp
from jax import lax

BLOCK = 512
BPD = 16
ITERS = 3
NB = 192
PAIR = 3
MOST = 36
N_DP = 12


def draw_gradients(key, part):
    folded = jax.random.fold_in(key, 11)
    row_key, col_key, own_key = jax.random.split(folded, 3)
    row_scale = jnp.exp(jax.random.uniform(row_key, (NB, BLOCK, 1), jnp.float32, 0.0, math.log(10.0)))
    col_scale = jnp.exp(jax.random.uniform(col_key, (NB, 1, BLOCK), jnp.float32, 0.0, math.log(10.0)))
    replica_ids = jnp.arange(N_DP, dtype=jnp.int32)[:, None]
    holder_ids = (jnp.arange(NB, dtype=jnp.int32) // BPD)[None, :]
    boost = jnp.where(replica_ids == holder_ids, 6.0, 1.0).astype(jnp.float32)[:, :, None, None]
    blended = jax.random.truncated_normal(own_key, -4.0, 4.0, (N_DP, NB, BLOCK, BLOCK), jnp.float32) * boost
    return (0.1 * blended * row_scale[None] * col_scale[None]).astype(jnp.bfloat16)


def draw_owners(key, part):
    folded = jax.random.fold_in(key, 5)
    busiest = jax.random.randint(jax.random.fold_in(folded, 1), (), 0, N_DP).astype(jnp.int32)

    def one_group(group_key):
        pick_key, mix_key = jax.random.split(group_key)
        tickets = jax.random.permutation(pick_key, (N_DP - 1) * PAIR)[:BPD - PAIR].astype(jnp.int32)
        others = tickets // PAIR
        others = others + (others >= busiest).astype(jnp.int32)
        assigned = jnp.concatenate([jnp.full((PAIR,), busiest, jnp.int32), others.astype(jnp.int32)])
        return assigned[jax.random.permutation(mix_key, BPD)]
    group_keys = jax.random.split(jax.random.fold_in(folded, 2), N_DP)
    return jax.vmap(one_group)(group_keys).reshape(NB).astype(jnp.int32)


def shard_levels(key, extent, shards, smallest, top_value):
    factor_of, own = 1.0, jax.random.fold_in(key, 6)
    for dim, parts in shards:
        draws = jnp.exp(jax.random.uniform(jax.random.fold_in(own, dim), (parts,), jnp.float32, smallest / len(shards), top_value / len(shards)))
        factor_of = factor_of * jnp.repeat(draws, extent[dim] // parts).reshape([-1 if axis == dim else 1 for axis in range(len(extent))])
    return factor_of


def centred(stream_key, shape, deviation, most, cuts=(), kind=jnp.bfloat16):
    result = deviation * jax.random.normal(stream_key, shape, jnp.float32)
    if cuts:
        result = result * shard_levels(stream_key, shape, cuts, -0.22, 0.18)
    return jnp.clip(result, -most, most).astype(kind)


def setup_inputs(seed: int = 0) -> dict:
    arg_keys = jax.random.split(jax.random.key(seed), 4)
    gradients = draw_gradients(jax.random.fold_in(arg_keys[3], 71), 0)
    momentum = centred(arg_keys[1], (N_DP, MOST, BLOCK, BLOCK), 6.0, 36.0, ((0, 12), (2, 64)))
    owners = draw_owners(jax.random.fold_in(arg_keys[3], 71), 0)
    return {"gradients": gradients, "momentum": momentum, "owners": owners}


decay_rate = 0.95
newton_a = 3.4445
newton_b = -4.775
newton_c = 2.0315
norm_eps = 1e-07

def ranks_of(labels):
    length = labels.shape[0]
    places = jnp.arange(length, dtype=jnp.int32)
    earlier = (labels[None, :] == labels[:, None]) & (places[None, :] < places[:, None])
    return lax.optimization_barrier(jnp.sum(earlier.astype(jnp.int32), axis=1)).astype(jnp.int32)

def iterate_block(blended):
    widened = blended.astype(jnp.float32)
    length_sq = jnp.sum(widened * widened)
    current = widened / (jnp.sqrt(length_sq) + norm_eps)
    scale_up = math.sqrt(BLOCK)
    highest = lax.Precision.HIGHEST
    for iteration in range(ITERS):
        squared = jnp.dot(current, current.T, precision=highest, preferred_element_type=jnp.float32)
        polynomial = newton_b * squared + newton_c * jnp.dot(squared, squared, precision=highest, preferred_element_type=jnp.float32)
        current = newton_a * current + jnp.dot(polynomial, current, precision=highest, preferred_element_type=jnp.float32)
    return current * scale_up

def reference(gradients, momentum, owners):
    accumulated = gradients[0].astype(jnp.float32)
    for replica in range(1, N_DP):
        accumulated = accumulated + gradients[replica].astype(jnp.float32)
    summed = accumulated.astype(jnp.bfloat16)
    slot_rank = ranks_of(owners)

    def one_block(block_id):
        widened_g = summed[block_id].astype(jnp.float32)
        widened_m = momentum[owners[block_id], slot_rank[block_id]].astype(jnp.float32)
        blended = (widened_g + decay_rate * (decay_rate * widened_m + widened_g)).astype(jnp.bfloat16)
        return iterate_block(blended)
    finished = lax.map(one_block, jnp.arange(NB, dtype=jnp.int32))
    empty = jnp.zeros((N_DP, MOST, BLOCK, BLOCK), jnp.float32)
    return empty.at[owners, slot_rank].set(finished)
```

```python
import math

import jax
import jax.numpy as jnp
from jax import lax
from jax.sharding import Mesh
from jax.sharding import PartitionSpec as P

ITERS = 3
PAIR = 3
TENSOR = ("ty", "tx", "tc")
HOLD = ("ty", "tc")
SPLIT = (8, 4, 2)


decay_rate = 0.95
newton_a = 3.4445
newton_b = -4.775
newton_c = 2.0315
norm_eps = 1e-07


def exchange(pieces, axes):
    return lax.all_to_all(pieces, axes, split_axis=0, concat_axis=0, tiled=True)


def shifted(pieces, step):
    count = lax.axis_size("dp")
    return lax.ppermute(pieces, "dp", [(i, (i + step) % count) for i in range(count)])


def ranks_of(labels):
    length = labels.shape[0]
    places = jnp.arange(length, dtype=jnp.int32)
    earlier = (labels[None, :] == labels[:, None]) & (places[None, :] < places[:, None])
    return jnp.sum(earlier.astype(jnp.int32), axis=1)


def sum_at_holder(chunks):
    wide = lambda piece: piece.astype(jnp.float32)
    narrow = lambda piece: piece.astype(jnp.bfloat16)
    at = lambda k: chunks[k % 12]
    size = chunks.shape[1]
    half = size // 2
    ahead = shifted(jnp.concatenate([at(5), at(-3), at(2)]), 1)
    behind = shifted(jnp.concatenate([at(-5), at(3), at(-2)]), -1)
    ahead_far = shifted(at(6)[:half], 2)
    behind_far = shifted(at(6)[half:], -2)
    blank = jnp.zeros(ahead_far.shape, jnp.float32)
    to_far = wide(at(4)) + wide(ahead[:size]) + wide(behind[size : 2 * size])
    to_far = narrow(to_far + jnp.concatenate([wide(ahead_far), blank]))
    from_far = wide(at(-4)) + wide(behind[:size]) + wide(ahead[size : 2 * size])
    from_far = narrow(from_far + jnp.concatenate([blank, wide(behind_far)]))
    to_near = narrow(wide(at(1)) + wide(ahead[2 * size :]))
    from_near = narrow(wide(at(-1)) + wide(behind[2 * size :]))
    far = wide(shifted(to_far, 4)) + wide(shifted(from_far, -4))
    near = wide(shifted(to_near, 1)) + wide(shifted(from_near, -1))
    return narrow(wide(at(0)) + far + near)


def iterate(block, first_row, rows):
    widened = block.astype(jnp.float32) * (1.0 + decay_rate)
    length = jnp.sqrt(jnp.sum(widened * widened)) + norm_eps
    current = widened / length
    scale_up = math.sqrt(block.shape[0])
    dot = lambda a, b: jnp.dot(a, b, preferred_element_type=jnp.float32)
    for iteration in range(ITERS):
        squared = lax.dot_general(
            current, current, (((1,), (1,)), ((), ())), preferred_element_type=jnp.float32
        )
        if iteration == ITERS - 1:
            mine = lax.dynamic_slice_in_dim(squared, first_row, rows)
            kept = lax.dynamic_slice_in_dim(current, first_row, rows)
        else:
            mine, kept = squared, current
        polynomial = newton_b * mine + newton_c * dot(mine, squared)
        current = newton_a * kept + dot(polynomial, current)
    return current * scale_up


def body(gradients, momentum, owners):
    dp_count = lax.axis_size("dp")
    my_group = lax.axis_index("dp")
    tx_count = lax.axis_size("tx")
    pieces = gradients[0]
    blocks_all, piece_rows, width = pieces.shape
    per_group = blocks_all // dp_count
    capacity = momentum.shape[1]
    places = jnp.arange(blocks_all, dtype=jnp.int32)
    slot_rank = ranks_of(owners)
    slot_ids = jnp.arange(capacity, dtype=jnp.int32)
    mine = owners == my_group
    weight = decay_rate * decay_rate / (1.0 + decay_rate)
    order = jnp.arange(dp_count, dtype=jnp.int32) + my_group
    order = jnp.where(order >= dp_count, order - dp_count, order)
    turned = jnp.take(pieces.reshape(dp_count, per_group, piece_rows, width), order, axis=0)
    turned_places = (order[:, None] * per_group + jnp.arange(per_group)[None, :]).reshape(-1)
    turned_mine = jnp.take(mine, turned_places)
    own_slot = jnp.take(jnp.where(mine, slot_rank, 0), turned_places)
    own_momentum = jnp.take(momentum[0], own_slot, axis=0).astype(jnp.float32)
    joined = turned.reshape(pieces.shape).astype(jnp.float32) + jnp.where(
        turned_mine[:, None, None], weight * own_momentum, 0.0
    )
    joined = joined.astype(jnp.bfloat16)
    held = sum_at_holder(joined.reshape(dp_count, per_group, piece_rows, width))
    hold_rows = lax.axis_size("ty")
    copies = held.reshape(hold_rows, 1, -1, piece_rows, width)
    copies = jnp.broadcast_to(copies, (hold_rows, tx_count, *copies.shape[2:]))
    whole = exchange(copies.reshape(-1, piece_rows, width), TENSOR)
    whole = whole.reshape(hold_rows, tx_count, -1, width).swapaxes(0, 1).reshape(-1, width)
    slab = whole.shape[0] // tx_count
    finished = iterate(whole, lax.axis_index("tx") * slab, slab)
    back = exchange(finished.astype(jnp.bfloat16).reshape(-1, piece_rows, width), HOLD)
    groups = jnp.arange(dp_count, dtype=jnp.int32)
    held_owner = lax.dynamic_slice_in_dim(owners, my_group * per_group, per_group)
    held_rank = ranks_of(held_owner)
    held_places = jnp.arange(per_group, dtype=jnp.int32)
    pair_ids = jnp.arange(PAIR, dtype=jnp.int32)
    matched = (held_owner[:, None, None] == groups[None, :, None]) & (
        held_rank[:, None, None] == pair_ids[None, None, :]
    )
    source = jnp.sum(jnp.where(matched, held_places[:, None, None], 0), axis=0).reshape(-1)
    outgoing = jnp.take(back, source, axis=0)
    incoming = exchange(outgoing, "dp")
    group_rank = ranks_of(owners * dp_count + places // per_group)
    position = places // per_group * PAIR + group_rank
    my_slots = mine[:, None] & (slot_rank[:, None] == slot_ids[None, :])
    occupied = jnp.any(my_slots, axis=0)
    arriving = jnp.sum(jnp.where(my_slots, position[:, None], 0), axis=0)
    chosen = jnp.take(incoming, arriving, axis=0).astype(jnp.float32)
    update = jnp.where(occupied[:, None, None], chosen, 0.0)
    return update[None]


def solution(mesh):
    split = Mesh(mesh.devices.reshape(mesh.shape["dp"], *SPLIT), ("dp", *TENSOR))
    in_specs = (P("dp", None, TENSOR, None), P("dp", None, TENSOR, None), P())
    out_specs = P("dp", None, TENSOR, None)
    return jax.shard_map(body, mesh=split, in_specs=in_specs, out_specs=out_specs, check_vma=False)
```

```python
import math

import jax
import jax.numpy as jnp
from jax import lax
from jax.experimental import pallas as pl
from jax.experimental.pallas import tpu as pltpu
from jax.sharding import Mesh
from jax.sharding import PartitionSpec as P

ITERS = 3
PAIR = 3
RING = ("da", "db")
TENSOR = ("ty", "tx", "tc")
HOLD = ("ty", "tc")
SPLIT = (8, 4, 2)
THIRDS = 3


decay_rate = 0.95
newton_a = 3.4445
newton_b = -4.775
newton_c = 2.0315
norm_eps = 1e-07


def exchange(pieces, axes):
    return lax.all_to_all(pieces, axes, split_axis=0, concat_axis=0, tiled=True)


def shifted(pieces, step):
    count = lax.axis_size(RING)
    return lax.ppermute(pieces, RING, [(i, (i + step) % count) for i in range(count)])


def ranks_of(labels):
    length = labels.shape[0]
    places = jnp.arange(length, dtype=jnp.int32)
    earlier = (labels[None, :] == labels[:, None]) & (places[None, :] < places[:, None])
    return jnp.sum(earlier.astype(jnp.int32), axis=1)


def join_kernel(where_ref, owners_ref, pieces_ref, momentum_ref, kept_ref, ahead_ref, behind_ref, found_ref, sems):
    weight = decay_rate * decay_rate / (1.0 + decay_rate)
    me, third = where_ref[0], where_ref[1]
    outs = (kept_ref, ahead_ref, behind_ref)
    quarters, _, per_group = pieces_ref.shape[:3]
    copies = []
    for step, out in enumerate(outs):
        which = lax.rem(third + step, THIRDS)
        for quarter in range(quarters):
            copies.append(
                pltpu.make_async_copy(
                    pieces_ref.at[quarter, which], out.at[quarter], sems.at[step * quarters + quarter]
                )
            )
    for copy in copies:
        copy.start()

    def look(place, count):
        found_ref[count] = place
        return count + (owners_ref[place] == me).astype(jnp.int32)

    total = lax.fori_loop(0, owners_ref.shape[0], look, 0, unroll=8)
    for copy in copies:
        copy.wait()

    def add(slot, carry):
        place = found_ref[slot]
        group = lax.div(place, per_group)
        inside = place - group * per_group
        quarter = lax.div(group, THIRDS)
        step = lax.rem(group - quarter * THIRDS - third + THIRDS, THIRDS)
        extra = weight * momentum_ref[slot].astype(jnp.float32)
        for index, out in enumerate(outs):

            @pl.when(step == index)
            def _():
                joined = out[quarter, inside].astype(jnp.float32) + extra
                out[quarter, inside] = joined.astype(out.dtype)

        return carry

    lax.fori_loop(0, total, add, 0)


def join_momentum(pieces, momentum, owners, where):
    quarters, thirds, *inside = pieces.shape
    out = jax.ShapeDtypeStruct((quarters, *inside), pieces.dtype)
    smem = pl.BlockSpec(memory_space=pltpu.SMEM)
    vmem = pl.BlockSpec(memory_space=pltpu.VMEM)
    return pl.pallas_call(
        join_kernel,
        out_shape=[out] * thirds,
        in_specs=[smem, smem, pl.BlockSpec(memory_space=pl.ANY), vmem],
        out_specs=[vmem] * thirds,
        scratch_shapes=[
            pltpu.SMEM((owners.shape[0] + 1,), jnp.int32),
            pltpu.SemaphoreType.DMA((thirds * quarters,)),
        ],
        cost_estimate=pl.CostEstimate(
            flops=2 * pieces.size, bytes_accessed=4 * pieces.size, transcendentals=0
        ),
        name="join_momentum",
    )(where, owners, pieces, momentum)


def iterate_kernel(slab_ref, pieces_ref, out_ref, wide_ref):
    count, piece_rows, width = pieces_ref.shape
    ty, tx, tc = SPLIT
    slab = count * piece_rows // tx
    square = jnp.zeros((piece_rows, width), jnp.float32)
    for y in range(ty):
        for x in range(tx):
            for c in range(tc):
                piece = pieces_ref[(y * tx + x) * tc + c].astype(jnp.float32)
                square = square + piece * piece
                row = x * slab + (y * tc + c) * piece_rows
                wide_ref[row : row + piece_rows, :] = piece
    blend = 1.0 + decay_rate
    total = jnp.sum(jnp.sum(square, axis=0, keepdims=True), axis=1, keepdims=True)
    scale = blend / (blend * jnp.sqrt(total) + norm_eps)
    wide_ref[...] = wide_ref[...] * scale

    def dot(left, right, across):
        return lax.dot_general(
            left, right, (((1,), (across,)), ((), ())), preferred_element_type=jnp.float32
        )

    narrow = lambda value: value.astype(jnp.bfloat16)
    for iteration in range(ITERS):
        last = iteration == ITERS - 1
        current = wide_ref[...]
        currents = narrow(current)
        if last:
            kept = wide_ref[pl.ds(slab_ref[0] * slab, slab), :]
            mine = dot(narrow(kept), currents, 1)
            squared = narrow(dot(currents, currents, 1))
            polynomial = newton_b * mine + newton_c * dot(narrow(mine), squared, 0)
        else:
            kept = current
            mine = dot(currents, currents, 1)
            squared = narrow(mine)
            polynomial = newton_b * mine + newton_c * dot(squared, squared, 0)
        following = newton_a * kept + dot(narrow(polynomial), currents, 0)
        if not last:
            wide_ref[...] = following
    result = following * math.sqrt(width)
    for piece in range(slab // piece_rows):
        rows = result[piece * piece_rows : (piece + 1) * piece_rows, :]
        out_ref[piece] = rows.astype(out_ref.dtype)


def iterate(pieces, slab_index):
    count, piece_rows, width = pieces.shape
    rows = count * piece_rows
    share = count // SPLIT[1]
    vmem = pl.BlockSpec(memory_space=pltpu.VMEM)
    return pl.pallas_call(
        iterate_kernel,
        out_shape=jax.ShapeDtypeStruct((share, piece_rows, width), pieces.dtype),
        in_specs=[pl.BlockSpec(memory_space=pltpu.SMEM), vmem],
        out_specs=vmem,
        scratch_shapes=[pltpu.VMEM((rows, width), jnp.float32)],
        cost_estimate=pl.CostEstimate(
            flops=3 * ITERS * 2 * rows * rows * width,
            bytes_accessed=4 * rows * width,
            transcendentals=0,
        ),
        name="iterate_block",
    )(slab_index, pieces)


def sum_at_holder(kept, ahead, behind):
    wide = lambda piece: piece.astype(jnp.float32)
    from_behind = shifted(ahead, 1)
    from_ahead = shifted(behind, -1)
    partial = (wide(kept) + wide(from_behind) + wide(from_ahead)).astype(jnp.bfloat16)
    return wide(exchange(partial, "da")).sum(axis=0).astype(jnp.bfloat16)


def body(gradients, momentum, owners):
    dp_count = lax.axis_size(RING)
    my_group = lax.axis_index(RING)
    tx_count = lax.axis_size("tx")
    pieces = gradients[0]
    blocks_all, piece_rows, width = pieces.shape
    per_group = blocks_all // dp_count
    capacity = momentum.shape[1]
    places = jnp.arange(blocks_all, dtype=jnp.int32)
    slot_rank = ranks_of(owners)
    slot_ids = jnp.arange(capacity, dtype=jnp.int32)
    mine = owners == my_group
    grouped = pieces.reshape(dp_count // THIRDS, THIRDS, per_group, piece_rows, width)
    where = jnp.stack([my_group, lax.axis_index("db")]).astype(jnp.int32)
    held = sum_at_holder(*join_momentum(grouped, momentum[0], owners, where))
    hold_rows = lax.axis_size("ty")
    copies = held.reshape(hold_rows, 1, -1, piece_rows, width)
    copies = jnp.broadcast_to(copies, (hold_rows, tx_count, *copies.shape[2:]))
    whole = exchange(copies.reshape(-1, piece_rows, width), TENSOR)
    slab_index = lax.axis_index("tx").astype(jnp.int32)[None]
    back = exchange(iterate(whole, slab_index), HOLD)
    groups = jnp.arange(dp_count, dtype=jnp.int32)
    held_owner = lax.dynamic_slice_in_dim(owners, my_group * per_group, per_group)
    held_rank = ranks_of(held_owner)
    held_places = jnp.arange(per_group, dtype=jnp.int32)
    pair_ids = jnp.arange(PAIR, dtype=jnp.int32)
    matched = (held_owner[:, None, None] == groups[None, :, None]) & (
        held_rank[:, None, None] == pair_ids[None, None, :]
    )
    source = jnp.sum(jnp.where(matched, held_places[:, None, None], 0), axis=0).reshape(-1)
    outgoing = jnp.take(back, source, axis=0, mode="clip")
    incoming = exchange(outgoing, RING)
    group_rank = ranks_of(owners * dp_count + places // per_group)
    position = places // per_group * PAIR + group_rank
    my_slots = mine[:, None] & (slot_rank[:, None] == slot_ids[None, :])
    occupied = jnp.any(my_slots, axis=0)
    arriving = jnp.sum(jnp.where(my_slots, position[:, None], 0), axis=0)
    chosen = jnp.take(incoming, arriving, axis=0, mode="clip").astype(jnp.float32)
    update = jnp.where(occupied[:, None, None], chosen, 0.0)
    return update[None]


def solution(mesh):
    split = Mesh(mesh.devices.reshape(-1, THIRDS, *SPLIT), (*RING, *TENSOR))
    in_specs = (P(RING, None, TENSOR, None), P(RING, None, TENSOR, None), P())
    out_specs = P(RING, None, TENSOR, None)
    return jax.shard_map(body, mesh=split, in_specs=in_specs, out_specs=out_specs, check_vma=False)
```

```python
import math

import jax
import jax.numpy as jnp
from jax import lax
from jax.experimental import pallas as pl
from jax.experimental.pallas import tpu as pltpu
from jax.sharding import Mesh
from jax.sharding import PartitionSpec as P

ITERS = 3
PAIR = 3
RING = ("da", "db")
TENSOR = ("ty", "tx", "tc")
HOLD = ("ty", "tc")
SPLIT = (8, 4, 2)
FOURTHS = 4
PARTS = 2
VMEM_LIMIT = 12 * 1024 * 1024


decay_rate = 0.95
newton_a = 3.4445
newton_b = -4.775
newton_c = 2.0315
norm_eps = 1e-07


def exchange(pieces, axes):
    return lax.all_to_all(pieces, axes, split_axis=0, concat_axis=0, tiled=True)


def shifted(pieces, step):
    count = lax.axis_size(RING)
    return lax.ppermute(pieces, RING, [(i, (i + step) % count) for i in range(count)])


def mirrored(pieces, step):
    count, cores = lax.axis_size(RING), lax.axis_size("tc")
    signs = [step if core else -step for core in range(cores)]
    pairs = [
        (i * cores + core, (i + signs[core]) % count * cores + core)
        for i in range(count)
        for core in range(cores)
    ]
    return lax.ppermute(pieces, (*RING, "tc"), pairs)


def ranks_of(labels):
    length = labels.shape[0]
    places = jnp.arange(length, dtype=jnp.int32)
    earlier = (labels[None, :] == labels[:, None]) & (places[None, :] < places[:, None])
    return jnp.sum(earlier.astype(jnp.int32), axis=1)


def join_kernel(owners_ref, pieces_ref, momentum_ref, *refs):
    *outs, found_ref, sems = refs
    weight = decay_rate * decay_rate / (1.0 + decay_rate)
    fourth = lax.axis_index(RING[1])
    me = lax.axis_index(RING[0]) * FOURTHS + fourth
    trios, _, per_group = pieces_ref.shape[:3]
    width = outs[0].shape[-1]
    copies = []
    for part in range(PARTS):
        columns = pl.ds(part * width, width)
        for step in (1, 3, 2, 0):
            which = lax.rem(fourth + step, FOURTHS)
            for trio in range(trios):
                copies.append(
                    pltpu.make_async_copy(
                        pieces_ref.at[trio, which, :, :, columns],
                        outs[part * FOURTHS + step].at[trio],
                        sems.at[len(copies)],
                    )
                )
    for copy in copies:
        copy.start()

    def look(place, count):
        found_ref[count] = place
        return count + (owners_ref[place] == me).astype(jnp.int32)

    total = lax.fori_loop(0, owners_ref.shape[0], look, 0, unroll=8)
    for copy in copies:
        copy.wait()

    def add(slot, carry):
        place = found_ref[slot]
        group = lax.div(place, per_group)
        inside = place - group * per_group
        trio = lax.div(group, FOURTHS)
        step = lax.rem(group - trio * FOURTHS - fourth + FOURTHS, FOURTHS)
        extra = weight * momentum_ref[slot].astype(jnp.float32)
        for index in range(FOURTHS):

            @pl.when(step == index)
            def _():
                for part in range(PARTS):
                    out = outs[part * FOURTHS + index]
                    term = extra[:, part * width : (part + 1) * width]
                    joined = out[trio, inside].astype(jnp.float32) + term
                    out[trio, inside] = joined.astype(out.dtype)

        return carry

    lax.fori_loop(0, total, add, 0)


def join_momentum(pieces, momentum, owners):
    trios, fourths, *inside, width = pieces.shape
    out = jax.ShapeDtypeStruct((trios, *inside, width // PARTS), pieces.dtype)
    vmem = pl.BlockSpec(memory_space=pltpu.VMEM)
    outs = pl.pallas_call(
        join_kernel,
        out_shape=[out] * (fourths * PARTS),
        in_specs=[
            pl.BlockSpec(memory_space=pltpu.SMEM),
            pl.BlockSpec(memory_space=pl.ANY),
            vmem,
        ],
        out_specs=[vmem] * (fourths * PARTS),
        scratch_shapes=[
            pltpu.SMEM((owners.shape[0] + 1,), jnp.int32),
            pltpu.SemaphoreType.DMA((fourths * PARTS * trios,)),
        ],
        cost_estimate=pl.CostEstimate(
            flops=2 * pieces.size, bytes_accessed=4 * pieces.size, transcendentals=0
        ),
        name="join_momentum",
        compiler_params=pltpu.CompilerParams(vmem_limit_bytes=VMEM_LIMIT),
    )(owners, pieces, momentum)
    return [outs[part * fourths : (part + 1) * fourths] for part in range(PARTS)]


def combine_kernel(kept_ref, one_ref, two_ref, three_ref, own_ref, ahead_ref, behind_ref):
    trios, blocks = kept_ref.shape[:2]
    me = lax.axis_index(RING[0])
    for step, out in enumerate((own_ref, ahead_ref, behind_ref)):
        which = lax.rem(me + step, trios)
        for block in range(blocks):
            total = kept_ref[which, block].astype(jnp.float32)
            for ref in (one_ref, two_ref, three_ref):
                total = total + ref[which, block].astype(jnp.float32)
            out[block] = total.astype(out.dtype)


def combine(kept, *arrived):
    trios, *inside = kept.shape
    vmem = pl.BlockSpec(memory_space=pltpu.VMEM)
    own = jax.ShapeDtypeStruct(tuple(inside), jnp.float32)
    sent = jax.ShapeDtypeStruct(tuple(inside), kept.dtype)
    return pl.pallas_call(
        combine_kernel,
        out_shape=[own, sent, sent],
        in_specs=[vmem] * 4,
        out_specs=[vmem] * 3,
        cost_estimate=pl.CostEstimate(
            flops=4 * kept.size, bytes_accessed=8 * kept.size, transcendentals=0
        ),
        name="combine_terms",
        compiler_params=pltpu.CompilerParams(vmem_limit_bytes=VMEM_LIMIT),
    )(kept, *arrived)


def spread_kernel(own_ref, ahead_ref, behind_ref, out_ref):
    _, tx, tc = SPLIT
    for block in range(own_ref.shape[0]):
        total = own_ref[block] + (
            ahead_ref[block].astype(jnp.float32) + behind_ref[block].astype(jnp.float32)
        )
        total = total.astype(out_ref.dtype)
        for x in range(tx):
            out_ref[(block // tc * tx + x) * tc + block % tc] = total


def spread(own, ahead, behind):
    blocks, *inside = own.shape
    vmem = pl.BlockSpec(memory_space=pltpu.VMEM)
    return pl.pallas_call(
        spread_kernel,
        out_shape=jax.ShapeDtypeStruct((blocks * SPLIT[1], *inside), ahead.dtype),
        in_specs=[vmem] * 3,
        out_specs=vmem,
        cost_estimate=pl.CostEstimate(
            flops=4 * own.size, bytes_accessed=8 * own.size, transcendentals=0
        ),
        name="spread_sum",
        compiler_params=pltpu.CompilerParams(vmem_limit_bytes=VMEM_LIMIT),
    )(own, ahead, behind)


def iterate_kernel(*refs):
    *ins, out_ref, wide_ref = refs
    count, piece_rows, part_width = ins[0].shape
    width = PARTS * part_width
    ty, tx, tc = SPLIT
    slab = count * piece_rows // tx
    square = jnp.zeros((piece_rows, part_width), jnp.float32)
    for part in range(PARTS):
        for y in range(ty):
            for x in range(tx):
                for c in range(tc):
                    piece = ins[part][(y * tx + x) * tc + c].astype(jnp.float32)
                    square = square + piece * piece
                    row = x * slab + (y * tc + c) * piece_rows
                    wide_ref[
                        row : row + piece_rows, part * part_width : (part + 1) * part_width
                    ] = piece
    blend = 1.0 + decay_rate
    total = jnp.sum(jnp.sum(square, axis=0, keepdims=True), axis=1, keepdims=True)
    scale = blend / (blend * jnp.sqrt(total) + norm_eps)
    wide_ref[...] = wide_ref[...] * scale

    def dot(left, right, across):
        return lax.dot_general(
            left, right, (((1,), (across,)), ((), ())), preferred_element_type=jnp.float32
        )

    narrow = lambda value: value.astype(jnp.bfloat16)
    for iteration in range(ITERS):
        last = iteration == ITERS - 1
        current = wide_ref[...]
        currents = narrow(current)
        if last:
            kept = wide_ref[pl.ds(lax.axis_index("tx") * slab, slab), :]
            mine = dot(narrow(kept), currents, 1)
            squared = narrow(dot(currents, currents, 1))
            polynomial = newton_b * mine + newton_c * dot(narrow(mine), squared, 0)
        else:
            kept = current
            mine = dot(currents, currents, 1)
            squared = narrow(mine)
            polynomial = newton_b * mine + newton_c * dot(squared, squared, 0)
        following = newton_a * kept + dot(narrow(polynomial), currents, 0)
        if not last:
            wide_ref[...] = following
    result = following * math.sqrt(width)
    for piece in range(slab // piece_rows):
        rows = result[piece * piece_rows : (piece + 1) * piece_rows, :]
        out_ref[piece] = rows.astype(out_ref.dtype)


def iterate(parts):
    count, piece_rows, part_width = parts[0].shape
    rows, width = count * piece_rows, part_width * PARTS
    vmem = pl.BlockSpec(memory_space=pltpu.VMEM)
    return pl.pallas_call(
        iterate_kernel,
        out_shape=jax.ShapeDtypeStruct((count // SPLIT[1], piece_rows, width), parts[0].dtype),
        in_specs=[vmem] * PARTS,
        out_specs=vmem,
        scratch_shapes=[pltpu.VMEM((rows, width), jnp.float32)],
        cost_estimate=pl.CostEstimate(
            flops=3 * ITERS * 2 * rows * rows * width,
            bytes_accessed=4 * rows * width,
            transcendentals=0,
        ),
        name="iterate_block",
        compiler_params=pltpu.CompilerParams(vmem_limit_bytes=VMEM_LIMIT),
    )(*parts)


def sum_at_holder(kept, ahead, two, behind):
    arrived = (shifted(ahead, 1), shifted(behind, -1), mirrored(two, 2))
    own, to_ahead, to_behind = combine(kept, *arrived)
    arrived = (shifted(to_ahead, FOURTHS), shifted(to_behind, -FOURTHS))
    return spread(own, *arrived)


def body(gradients, momentum, owners):
    dp_count = lax.axis_size(RING)
    my_group = lax.axis_index(RING)
    pieces = gradients[0]
    blocks_all, piece_rows, width = pieces.shape
    per_group = blocks_all // dp_count
    capacity = momentum.shape[1]
    places = jnp.arange(blocks_all, dtype=jnp.int32)
    slot_rank = ranks_of(owners)
    slot_ids = jnp.arange(capacity, dtype=jnp.int32)
    mine = owners == my_group
    grouped = pieces.reshape(dp_count // FOURTHS, FOURTHS, per_group, piece_rows, width)
    joined = join_momentum(grouped, momentum[0], owners)
    whole = []
    for part in joined:
        whole.append(exchange(sum_at_holder(*part), TENSOR))
    back = exchange(iterate(whole), HOLD)
    groups = jnp.arange(dp_count, dtype=jnp.int32)
    held_owner = lax.dynamic_slice_in_dim(owners, my_group * per_group, per_group)
    held_rank = ranks_of(held_owner)
    held_places = jnp.arange(per_group, dtype=jnp.int32)
    pair_ids = jnp.arange(PAIR, dtype=jnp.int32)
    matched = (held_owner[:, None, None] == groups[None, :, None]) & (
        held_rank[:, None, None] == pair_ids[None, None, :]
    )
    source = jnp.sum(jnp.where(matched, held_places[:, None, None], 0), axis=0).reshape(-1)
    incoming = exchange(jnp.take(back, source, axis=0, mode="clip"), RING)
    group_rank = ranks_of(owners * dp_count + places // per_group)
    position = places // per_group * PAIR + group_rank
    my_slots = mine[:, None] & (slot_rank[:, None] == slot_ids[None, :])
    occupied = jnp.any(my_slots, axis=0)
    arriving = jnp.sum(jnp.where(my_slots, position[:, None], 0), axis=0)
    chosen = jnp.take(incoming, arriving, axis=0, mode="clip").astype(jnp.float32)
    update = jnp.where(occupied[:, None, None], chosen, 0.0)
    return update[None]


def solution(mesh):
    split = Mesh(mesh.devices.reshape(-1, FOURTHS, *SPLIT), (*RING, *TENSOR))
    in_specs = (P(RING, None, TENSOR, None), P(RING, None, TENSOR, None), P())
    out_specs = P(RING, None, TENSOR, None)
    return jax.shard_map(body, mesh=split, in_specs=in_specs, out_specs=out_specs, check_vma=False)
```

```python
import math

import jax
import jax.numpy as jnp
from jax import lax
from jax.experimental import pallas as pl
from jax.experimental.pallas import tpu as pltpu
from jax.sharding import Mesh
from jax.sharding import PartitionSpec as P

ITERS = 3
PAIR = 3
RING = ("da", "db")
TENSOR = ("yb", "ya", "tx", "tc")
CHIPS = ("yb", "ya", "tx")
HOLD = ("ya", "tx")
SPLIT = (2, 4, 4, 2)
FOURTHS = 4
VMEM_LIMIT = 12 * 1024 * 1024


decay_rate = 0.95
newton_a = 3.4445
newton_b = -4.775
newton_c = 2.0315
norm_eps = 1e-07


def exchange(pieces, axes):
    return lax.all_to_all(pieces, axes, split_axis=0, concat_axis=0, tiled=True)


def mirrored(pieces, step):
    count, cores = lax.axis_size(RING), lax.axis_size("tc")
    pairs = [
        (i * cores + core, (i + (step if core else -step)) % count * cores + core)
        for i in range(count)
        for core in range(cores)
    ]
    return lax.ppermute(pieces, (*RING, "tc"), pairs)


def ranks_of(labels):
    length = labels.shape[0]
    places = jnp.arange(length, dtype=jnp.int32)
    earlier = (labels[None, :] == labels[:, None]) & (places[None, :] < places[:, None])
    return jnp.sum(earlier.astype(jnp.int32), axis=1)


def call(kernel, outs, ins, scratch=(), flops=0, size=0, limit=VMEM_LIMIT):
    vmem = pl.BlockSpec(memory_space=pltpu.VMEM)
    return pl.pallas_call(
        kernel,
        out_shape=outs,
        in_specs=[vmem if space is None else pl.BlockSpec(memory_space=space) for space in ins],
        out_specs=jax.tree.map(lambda _: vmem, outs),
        scratch_shapes=list(scratch),
        cost_estimate=pl.CostEstimate(flops=flops, bytes_accessed=size, transcendentals=0),
        compiler_params=pltpu.CompilerParams(vmem_limit_bytes=limit),
    )


def join_kernel(owners_ref, pieces_ref, momentum_ref, *refs):
    *outs, held_owners, found_ref, slots_ref, sems = refs
    fars, owns = outs[:FOURTHS], outs[FOURTHS:]
    weight = decay_rate * decay_rate / (1.0 + decay_rate)
    trios, fourths, per_group = pieces_ref.shape[:3]
    count = trios * fourths
    me = lax.axis_index(RING[0]) * fourths + lax.axis_index(RING[1])
    side = 2 * lax.axis_index("tc") - 1
    collectors = [
        lax.rem(me + away * side + count, count) for away in (0, 1, -1, 2)
    ]
    trio_of = [lax.div(place, fourths) for place in collectors]
    fourth_of = [lax.rem(place, fourths) for place in collectors]
    table = pltpu.make_async_copy(owners_ref, held_owners, sems.at[0])
    table.start()
    slots = pltpu.make_async_copy(momentum_ref, slots_ref, sems.at[1])
    slots.start()
    copies = []
    for step in (1, 2, 3, 0):
        for rel in range(trios):
            target = owns[step] if rel == 0 else fars[step].at[rel - 1]
            source = pieces_ref.at[lax.rem(trio_of[step] + rel, trios), fourth_of[step]]
            copies.append(pltpu.make_async_copy(source, target, sems.at[2 + len(copies)]))
    for copy in copies:
        copy.start()
    table.wait()

    def look(place, found):
        found_ref[found] = place
        return found + (held_owners[place] == me).astype(jnp.int32)

    total = lax.fori_loop(0, held_owners.shape[0], look, 0, unroll=8)
    slots.wait()
    for copy in copies:
        copy.wait()

    def add(slot, carry):
        place = found_ref[slot]
        group = lax.div(place, per_group)
        inside = place - group * per_group
        trio = lax.div(group, fourths)
        fourth = group - trio * fourths
        extra = weight * slots_ref[slot].astype(jnp.float32)
        for step in range(fourths):
            rel = lax.rem(trio - trio_of[step] + trios, trios)

            @pl.when((fourth == fourth_of[step]) & (rel == 0))
            def _():
                own = owns[step]
                own[inside] = (own[inside].astype(jnp.float32) + extra).astype(own.dtype)

            @pl.when((fourth == fourth_of[step]) & (rel != 0))
            def _():
                far = fars[step]
                joined = far[rel - 1, inside].astype(jnp.float32) + extra
                far[rel - 1, inside] = joined.astype(far.dtype)

        return carry

    lax.fori_loop(0, total, add, 0)


def join_momentum(pieces, momentum, owners):
    trios, fourths, *inside = pieces.shape
    far = jax.ShapeDtypeStruct((trios - 1, *inside), pieces.dtype)
    own = jax.ShapeDtypeStruct(tuple(inside), pieces.dtype)
    outs = call(
        join_kernel,
        [far] * fourths + [own] * fourths,
        [pltpu.HBM] * 3,
        [
            pltpu.SMEM(owners.shape, jnp.int32),
            pltpu.SMEM((owners.shape[0] + 1,), jnp.int32),
            pltpu.VMEM(momentum.shape, momentum.dtype),
            pltpu.SemaphoreType.DMA((2 + trios * fourths,)),
        ],
        2 * pieces.size,
        4 * pieces.size,
    )(owners, pieces, momentum)
    return outs[:fourths], outs[fourths:]


def combine_kernel(*refs):
    *terms, first_ref, second_ref = refs
    core = lax.axis_index("tc")
    for which, out in ((1 - core, first_ref), (core, second_ref)):
        for block in range(out.shape[0]):
            total = terms[0][which, block].astype(jnp.float32)
            for term in terms[1:]:
                total = total + term[which, block].astype(jnp.float32)
            out[block] = total.astype(out.dtype)


def combine(terms):
    out = jax.ShapeDtypeStruct(terms[0].shape[1:], terms[0].dtype)
    size = len(terms) * terms[0].size
    return call(combine_kernel, [out] * 2, [None] * len(terms), (), size, 2 * size)(*terms)


def spread_kernel(*refs):
    *terms, out_ref = refs
    blocks = terms[0].shape[0]
    for block in range(blocks):
        total = terms[0][block].astype(jnp.float32)
        for term in terms[1:]:
            total = total + term[block].astype(jnp.float32)
        total = total.astype(out_ref.dtype)
        for copy in range(SPLIT[0]):
            out_ref[copy * blocks + block] = total


def spread(terms):
    blocks, *inside = terms[0].shape
    out = jax.ShapeDtypeStruct((blocks * SPLIT[0], *inside), terms[0].dtype)
    size = len(terms) * terms[0].size
    return call(spread_kernel, out, [None] * len(terms), (), size, 2 * size)(*terms)


def sum_at_holder(fars, owns):
    away = (1, -1, 2)
    arrived = [mirrored(term, step) for term, step in zip(fars[1:], away)]
    stayed = [mirrored(term, step) for term, step in zip(owns[1:], away)]
    first, second = combine([fars[0], *arrived])
    sums = [mirrored(first, FOURTHS), mirrored(second, -FOURTHS)]
    return spread([owns[0], *stayed, *sums])


def iterate_kernel(mine_ref, other_ref, out_ref, wide_ref):
    count, piece_rows, width = mine_ref.shape
    slab = count * piece_rows // SPLIT[0]
    square = jnp.zeros((piece_rows, width), jnp.float32)
    for side, ref in enumerate((mine_ref, other_ref)):
        for index in range(count):
            piece = ref[index].astype(jnp.float32)
            square = square + piece * piece
            row = (side * count + index) * piece_rows
            wide_ref[row : row + piece_rows, :] = piece
    blend = 1.0 + decay_rate
    total = jnp.sum(jnp.sum(square, axis=0, keepdims=True), axis=1, keepdims=True)
    scale = blend / (blend * jnp.sqrt(total) + norm_eps)
    wide_ref[...] = wide_ref[...] * scale

    def dot(left, right, across):
        return lax.dot_general(
            left, right, (((1,), (across,)), ((), ())), preferred_element_type=jnp.float32
        )

    narrow = lambda value: value.astype(jnp.bfloat16)
    for iteration in range(ITERS):
        last = iteration == ITERS - 1
        current = wide_ref[...]
        currents = narrow(current)
        if last:
            kept = wide_ref[pl.ds(lax.axis_index("yb") * slab, slab), :]
            mine = dot(narrow(kept), currents, 1)
            squared = narrow(dot(currents, currents, 1))
            polynomial = newton_b * mine + newton_c * dot(narrow(mine), squared, 0)
        else:
            kept = current
            mine = dot(currents, currents, 1)
            squared = narrow(mine)
            polynomial = newton_b * mine + newton_c * dot(squared, squared, 0)
        following = newton_a * kept + dot(narrow(polynomial), currents, 0)
        if not last:
            wide_ref[...] = following
    result = following * math.sqrt(width)
    for piece in range(slab // piece_rows):
        rows = result[piece * piece_rows : (piece + 1) * piece_rows, :]
        out_ref[piece] = rows.astype(out_ref.dtype)


def iterate(mine, other):
    count, piece_rows, width = mine.shape
    rows = 2 * count * piece_rows
    out = jax.ShapeDtypeStruct((count // SPLIT[0], piece_rows, width), mine.dtype)
    return call(
        iterate_kernel,
        out,
        [None] * 2,
        [pltpu.VMEM((rows, width), jnp.float32)],
        3 * ITERS * 2 * rows * rows * width,
        4 * rows * width,
    )(mine, other)


def pick_kernel(index_ref, limit_ref, table_ref, out_ref):
    for place in range(out_ref.shape[0]):
        row = table_ref[index_ref[place]].astype(out_ref.dtype)
        out_ref[place] = jnp.where(place < limit_ref[0], row, jnp.zeros_like(row))


def pick(table, index, limit, dtype):
    out = jax.ShapeDtypeStruct((*index.shape, *table.shape[1:]), dtype)
    ins = [pltpu.SMEM, pltpu.SMEM, None]
    size = 4 * math.prod(out.shape)
    return call(pick_kernel, out, ins, (), size // 4, size)(index, limit[None], table)


def body(gradients, momentum, owners):
    dp_count = lax.axis_size(RING)
    my_group = lax.axis_index(RING)
    pieces = gradients[0]
    blocks_all, piece_rows, width = pieces.shape
    per_group = blocks_all // dp_count
    capacity = momentum.shape[1]
    places = jnp.arange(blocks_all, dtype=jnp.int32)
    slot_rank = ranks_of(owners)
    slot_ids = jnp.arange(capacity, dtype=jnp.int32)
    mine = owners == my_group
    grouped = pieces.reshape(dp_count // FOURTHS, FOURTHS, per_group, piece_rows, width)
    held = sum_at_holder(*join_momentum(grouped, momentum[0], owners))
    arrived = exchange(held, CHIPS)
    partner = lax.ppermute(arrived, "tc", [(0, 1), (1, 0)])
    back = exchange(iterate(arrived, partner), HOLD)
    groups = jnp.arange(dp_count, dtype=jnp.int32)
    held_owner = lax.dynamic_slice_in_dim(owners, my_group * per_group, per_group)
    held_rank = ranks_of(held_owner)
    held_places = jnp.arange(per_group, dtype=jnp.int32)
    pair_ids = jnp.arange(PAIR, dtype=jnp.int32)
    matched = (held_owner[:, None, None] == groups[None, :, None]) & (
        held_rank[:, None, None] == pair_ids[None, None, :]
    )
    source = jnp.sum(jnp.where(matched, held_places[:, None, None], 0), axis=0).reshape(-1)
    everything = jnp.asarray(source.shape[0], jnp.int32)
    incoming = exchange(pick(back, source, everything, back.dtype), RING)
    group_rank = ranks_of(owners * dp_count + places // per_group)
    position = places // per_group * PAIR + group_rank
    my_slots = mine[:, None] & (slot_rank[:, None] == slot_ids[None, :])
    arriving = jnp.sum(jnp.where(my_slots, position[:, None], 0), axis=0)
    filled = jnp.sum(mine.astype(jnp.int32))
    return pick(incoming, arriving, filled, jnp.float32)[None]


def solution(mesh):
    split = Mesh(mesh.devices.reshape(-1, FOURTHS, *SPLIT), (*RING, *TENSOR))
    in_specs = (P(RING, None, TENSOR, None), P(RING, None, TENSOR, None), P())
    out_specs = P(RING, None, TENSOR, None)
    return jax.shard_map(body, mesh=split, in_specs=in_specs, out_specs=out_specs, check_vma=False)
```

```python
import math

import jax
import jax.numpy as jnp
from jax import lax
from jax.experimental import pallas as pl
from jax.experimental.pallas import tpu as pltpu
from jax.sharding import Mesh
from jax.sharding import PartitionSpec as P

ITERS = 3
PAIR = 3
RING = ("da", "db")
TENSOR = ("yb", "ya", "tx", "tc")
CHIPS = ("yb", "ya", "tx")
HOLD = ("ya", "tx")
SPLIT = (2, 4, 4, 2)
FOURTHS = 4
VMEM_LIMIT = 12 * 1024 * 1024
JOIN_LIMIT = 65_400_000


decay_rate = 0.95
newton_a = 3.4445
newton_b = -4.775
newton_c = 2.0315
norm_eps = 1e-07


def exchange(pieces, axes):
    return lax.all_to_all(pieces, axes, split_axis=0, concat_axis=0, tiled=True)


def mirrored(pieces, step):
    count, cores = lax.axis_size(RING), lax.axis_size("tc")
    pairs = [
        (i * cores + core, (i + (step if core else -step)) % count * cores + core)
        for i in range(count)
        for core in range(cores)
    ]
    return lax.ppermute(pieces, (*RING, "tc"), pairs)


def ranks_of(labels):
    length = labels.shape[0]
    places = jnp.arange(length, dtype=jnp.int32)
    earlier = (labels[None, :] == labels[:, None]) & (places[None, :] < places[:, None])
    return jnp.sum(earlier.astype(jnp.int32), axis=1)


def call(kernel, outs, ins, scratch=(), flops=0, size=0, limit=VMEM_LIMIT):
    vmem = pl.BlockSpec(memory_space=pltpu.VMEM)
    return pl.pallas_call(
        kernel,
        out_shape=outs,
        in_specs=[vmem if space is None else pl.BlockSpec(memory_space=space) for space in ins],
        out_specs=jax.tree.map(lambda _: vmem, outs),
        scratch_shapes=list(scratch),
        cost_estimate=pl.CostEstimate(flops=flops, bytes_accessed=size, transcendentals=0),
        compiler_params=pltpu.CompilerParams(vmem_limit_bytes=limit),
    )


def join_kernel(owners_ref, pieces_ref, momentum_ref, *refs):
    *outs, held_owners, found_ref, bounds_ref, slots_ref, sems = refs
    fars, owns = outs[:FOURTHS], outs[FOURTHS:]
    weight = decay_rate * decay_rate / (1.0 + decay_rate)
    trios, fourths, per_group = pieces_ref.shape[:3]
    count = trios * fourths
    me = lax.axis_index(RING[0]) * fourths + lax.axis_index(RING[1])
    side = 2 * lax.axis_index("tc") - 1
    collectors = [
        lax.rem(me + away * side + count, count) for away in (0, 1, -1, 2)
    ]
    trio_of = [lax.div(place, fourths) for place in collectors]
    fourth_of = [lax.rem(place, fourths) for place in collectors]
    table = pltpu.make_async_copy(owners_ref, held_owners, sems.at[0])
    table.start()
    slots = pltpu.make_async_copy(momentum_ref, slots_ref, sems.at[1])
    slots.start()
    copies = []
    for step in (1, 2, 3, 0):
        for rel in range(trios):
            target = owns[step] if rel == 0 else fars[step].at[rel - 1]
            source = pieces_ref.at[lax.rem(trio_of[step] + rel, trios), fourth_of[step]]
            copies.append(pltpu.make_async_copy(source, target, sems.at[2 + len(copies)]))
    for copy in copies:
        copy.start()
    table.wait()

    found = jnp.int32(0)
    for group in range(count):
        bounds_ref[group] = found
        for inside in range(per_group):
            found_ref[found] = inside
            found = found + (held_owners[group * per_group + inside] == me).astype(jnp.int32)
    bounds_ref[count] = found
    slots.wait()
    for index, copy in enumerate(copies):
        step, rel = (1, 2, 3, 0)[index // trios], index % trios
        target = owns[step] if rel == 0 else fars[step].at[rel - 1]
        group = lax.rem(trio_of[step] + rel, trios) * fourths + fourth_of[step]
        copy.wait()

        def add(slot, carry, target=target):
            inside = found_ref[slot]
            extra = weight * slots_ref[slot].astype(jnp.float32)
            target[inside] = (target[inside].astype(jnp.float32) + extra).astype(target.dtype)
            return carry

        lax.fori_loop(bounds_ref[group], bounds_ref[group + 1], add, 0)


def join_momentum(pieces, momentum, owners):
    trios, fourths, *inside = pieces.shape
    far = jax.ShapeDtypeStruct((trios - 1, *inside), pieces.dtype)
    own = jax.ShapeDtypeStruct(tuple(inside), pieces.dtype)
    outs = call(
        join_kernel,
        [far] * fourths + [own] * fourths,
        [pltpu.HBM] * 3,
        [
            pltpu.SMEM(owners.shape, jnp.int32),
            pltpu.SMEM((owners.shape[0] + 1,), jnp.int32),
            pltpu.SMEM((trios * fourths + 1,), jnp.int32),
            pltpu.VMEM(momentum.shape, momentum.dtype),
            pltpu.SemaphoreType.DMA((2 + trios * fourths,)),
        ],
        2 * pieces.size,
        4 * pieces.size,
        JOIN_LIMIT,
    )(owners, pieces, momentum)
    return outs[:fourths], outs[fourths:]


def combine_kernel(*refs):
    *terms, first_ref, second_ref = refs
    core = lax.axis_index("tc")
    for which, out in ((1 - core, first_ref), (core, second_ref)):
        for block in range(out.shape[0]):
            total = terms[0][which, block].astype(jnp.float32)
            for term in terms[1:]:
                total = total + term[which, block].astype(jnp.float32)
            out[block] = total.astype(out.dtype)


def combine(terms):
    out = jax.ShapeDtypeStruct(terms[0].shape[1:], terms[0].dtype)
    size = len(terms) * terms[0].size
    return call(combine_kernel, [out] * 2, [None] * len(terms), (), size, 2 * size)(*terms)


def spread_kernel(*refs):
    *terms, out_ref = refs
    blocks = terms[0].shape[0]
    for block in range(blocks):
        total = terms[0][block].astype(jnp.float32)
        for term in terms[1:]:
            total = total + term[block].astype(jnp.float32)
        total = total.astype(out_ref.dtype)
        for copy in range(SPLIT[0]):
            out_ref[copy * blocks + block] = total


def spread(terms):
    blocks, *inside = terms[0].shape
    out = jax.ShapeDtypeStruct((blocks * SPLIT[0], *inside), terms[0].dtype)
    size = len(terms) * terms[0].size
    return call(spread_kernel, out, [None] * len(terms), (), size, 2 * size)(*terms)


def sum_at_holder(fars, owns):
    away = (1, -1, 2)
    arrived = [mirrored(term, step) for term, step in zip(fars[1:], away)]
    stayed = [mirrored(term, step) for term, step in zip(owns[1:], away)]
    first, second = combine([fars[0], *arrived])
    sums = [mirrored(first, FOURTHS), mirrored(second, -FOURTHS)]
    return spread([owns[0], *stayed, *sums])


def iterate_kernel(mine_ref, other_ref, out_ref, wide_ref):
    count, piece_rows, width = mine_ref.shape
    slab = count * piece_rows // SPLIT[0]
    square = jnp.zeros((piece_rows, width), jnp.float32)
    for side, ref in enumerate((mine_ref, other_ref)):
        for index in range(count):
            piece = ref[index].astype(jnp.float32)
            square = square + piece * piece
            row = (side * count + index) * piece_rows
            wide_ref[row : row + piece_rows, :] = piece
    blend = 1.0 + decay_rate
    total = jnp.sum(jnp.sum(square, axis=0, keepdims=True), axis=1, keepdims=True)
    scale = blend / (blend * jnp.sqrt(total) + norm_eps)
    wide_ref[...] = wide_ref[...] * scale

    def dot(left, right, across):
        return lax.dot_general(
            left, right, (((1,), (across,)), ((), ())), preferred_element_type=jnp.float32
        )

    narrow = lambda value: value.astype(jnp.bfloat16)
    for iteration in range(ITERS):
        last = iteration == ITERS - 1
        current = wide_ref[...]
        currents = narrow(current)
        if last:
            kept = wide_ref[pl.ds(lax.axis_index("yb") * slab, slab), :]
            mine = dot(narrow(kept), currents, 1)
            squared = narrow(dot(currents, currents, 1))
            polynomial = newton_b * mine + newton_c * dot(narrow(mine), squared, 0)
        else:
            kept = current
            mine = dot(currents, currents, 1)
            squared = narrow(mine)
            polynomial = newton_b * mine + newton_c * dot(squared, squared, 0)
        following = newton_a * kept + dot(narrow(polynomial), currents, 0)
        if not last:
            wide_ref[...] = following
    result = following * math.sqrt(width)
    for piece in range(slab // piece_rows):
        rows = result[piece * piece_rows : (piece + 1) * piece_rows, :]
        out_ref[piece] = rows.astype(out_ref.dtype)


def iterate(mine, other):
    count, piece_rows, width = mine.shape
    rows = 2 * count * piece_rows
    out = jax.ShapeDtypeStruct((count // SPLIT[0], piece_rows, width), mine.dtype)
    return call(
        iterate_kernel,
        out,
        [None] * 2,
        [pltpu.VMEM((rows, width), jnp.float32)],
        3 * ITERS * 2 * rows * rows * width,
        4 * rows * width,
    )(mine, other)


def body(gradients, momentum, owners):
    dp_count = lax.axis_size(RING)
    my_group = lax.axis_index(RING)
    pieces = gradients[0]
    blocks_all, piece_rows, width = pieces.shape
    per_group = blocks_all // dp_count
    capacity = momentum.shape[1]
    places = jnp.arange(blocks_all, dtype=jnp.int32)
    slot_rank = ranks_of(owners)
    slot_ids = jnp.arange(capacity, dtype=jnp.int32)
    mine = owners == my_group
    grouped = pieces.reshape(dp_count // FOURTHS, FOURTHS, per_group, piece_rows, width)
    held = sum_at_holder(*join_momentum(grouped, momentum[0], owners))
    arrived = exchange(held, CHIPS)
    partner = lax.ppermute(arrived, "tc", [(0, 1), (1, 0)])
    back = exchange(iterate(arrived, partner), HOLD)
    groups = jnp.arange(dp_count, dtype=jnp.int32)
    held_owner = lax.dynamic_slice_in_dim(owners, my_group * per_group, per_group)
    held_rank = ranks_of(held_owner)
    held_places = jnp.arange(per_group, dtype=jnp.int32)
    pair_ids = jnp.arange(PAIR, dtype=jnp.int32)
    matched = (held_owner[:, None, None] == groups[None, :, None]) & (
        held_rank[:, None, None] == pair_ids[None, None, :]
    )
    source = jnp.sum(jnp.where(matched, held_places[:, None, None], 0), axis=0).reshape(-1)
    incoming = exchange(jnp.take(back, source, axis=0, mode="clip"), RING)
    group_rank = ranks_of(owners * dp_count + places // per_group)
    position = places // per_group * PAIR + group_rank
    my_slots = mine[:, None] & (slot_rank[:, None] == slot_ids[None, :])
    arriving = jnp.sum(jnp.where(my_slots, position[:, None], 0), axis=0)
    occupied = jnp.any(my_slots, axis=0)
    chosen = jnp.take(incoming, arriving, axis=0, mode="clip").astype(jnp.float32)
    return jnp.where(occupied[:, None, None], chosen, 0.0)[None]


def solution(mesh):
    split = Mesh(mesh.devices.reshape(-1, FOURTHS, *SPLIT), (*RING, *TENSOR))
    in_specs = (P(RING, None, TENSOR, None), P(RING, None, TENSOR, None), P())
    out_specs = P(RING, None, TENSOR, None)
    return jax.shard_map(body, mesh=split, in_specs=in_specs, out_specs=out_specs, check_vma=False)
```

```python
import math

import jax
import jax.numpy as jnp
from jax import lax
from jax.experimental import pallas as pl
from jax.experimental.pallas import tpu as pltpu
from jax.sharding import Mesh
from jax.sharding import PartitionSpec as P

ITERS = 3
PAIR = 3
TENSOR = ("yb", "ya", "tx", "tc")
CHIPS = ("yb", "ya", "tx")
HOLD = ("ya", "tx")
SPLIT = (2, 4, 4, 2)
VMEM_LIMIT = 12 * 1024 * 1024
PLACES = ((5, -3, 2), (-5, 3, -2), (6,), (4, -4, 1, -1), (0,))


decay_rate = 0.95
newton_a = 3.4445
newton_b = -4.775
newton_c = 2.0315
norm_eps = 1e-07


def exchange(pieces, axes):
    return lax.all_to_all(pieces, axes, split_axis=0, concat_axis=0, tiled=True)


def mirrored(pieces, step):
    count, cores = lax.axis_size("dp"), lax.axis_size("tc")
    pairs = [
        (i * cores + core, (i + (step if core else -step)) % count * cores + core)
        for i in range(count)
        for core in range(cores)
    ]
    return lax.ppermute(pieces, ("dp", "tc"), pairs)


def ranks_of(labels):
    length = labels.shape[0]
    places = jnp.arange(length, dtype=jnp.int32)
    earlier = (labels[None, :] == labels[:, None]) & (places[None, :] < places[:, None])
    return jnp.sum(earlier.astype(jnp.int32), axis=1)


def call(kernel, name, outs, ins, scratch=(), flops=0, size=0, limit=VMEM_LIMIT):
    vmem = pl.BlockSpec(memory_space=pltpu.VMEM)
    return pl.pallas_call(
        kernel,
        out_shape=outs,
        in_specs=[vmem if space is None else pl.BlockSpec(memory_space=space) for space in ins],
        out_specs=jax.tree.map(lambda _: vmem, outs),
        scratch_shapes=list(scratch),
        cost_estimate=pl.CostEstimate(flops=flops, bytes_accessed=size, transcendentals=0),
        compiler_params=pltpu.CompilerParams(vmem_limit_bytes=limit),
        name=name,
    )


def join_kernel(owners_ref, pieces_ref, momentum_ref, *refs):
    *outs, held_owners, found_ref, bounds_ref, slots_ref, sems = refs
    weight = decay_rate * decay_rate / (1.0 + decay_rate)
    count, per_group = pieces_ref.shape[:2]
    me = lax.axis_index("dp")
    side = 2 * lax.axis_index("tc") - 1
    table = pltpu.make_async_copy(owners_ref, held_owners, sems.at[0])
    table.start()
    slots = pltpu.make_async_copy(momentum_ref, slots_ref, sems.at[1])
    slots.start()
    jobs = []
    for out, aways in zip(outs, PLACES):
        for index, away in enumerate(aways):
            group = lax.rem(me + away * side + count, count)
            copy = pltpu.make_async_copy(
                pieces_ref.at[group], out.at[index], sems.at[2 + len(jobs)]
            )
            jobs.append((copy, group, out.at[index]))
    for copy, _, _ in jobs:
        copy.start()
    table.wait()
    found = jnp.int32(0)
    for group in range(count):
        bounds_ref[group] = found
        for inside in range(per_group):
            found_ref[found] = inside
            found = found + (held_owners[group * per_group + inside] == me).astype(jnp.int32)
    bounds_ref[count] = found
    slots.wait()
    for copy, group, target in jobs:
        copy.wait()

        def add(slot, carry, target=target):
            inside = found_ref[slot]
            extra = weight * slots_ref[slot].astype(jnp.float32)
            target[inside] = (target[inside].astype(jnp.float32) + extra).astype(target.dtype)
            return carry

        lax.fori_loop(bounds_ref[group], bounds_ref[group + 1], add, 0)


def join_momentum(pieces, momentum, owners):
    count, *inside = pieces.shape
    outs = [jax.ShapeDtypeStruct((len(aways), *inside), pieces.dtype) for aways in PLACES]
    scratch = [
        pltpu.SMEM(owners.shape, jnp.int32),
        pltpu.SMEM((owners.shape[0] + 1,), jnp.int32),
        pltpu.SMEM((count + 1,), jnp.int32),
        pltpu.VMEM(momentum.shape, momentum.dtype),
        pltpu.SemaphoreType.DMA((2 + count,)),
    ]
    hbm = [pltpu.with_memory_space_constraint(x, pltpu.HBM) for x in (owners, pieces, momentum)]
    size = 2 * pieces.size
    return call(join_kernel, "join_momentum", outs, [pltpu.HBM] * 3, scratch, size, 2 * size)(*hbm)


def combine_kernel(one_ref, two_ref, three_ref, kept_ref, *outs):
    wide = lambda ref, index, block: ref[index, block].astype(jnp.float32)
    for block in range(kept_ref.shape[1]):
        ahead = wide(one_ref, 0, block) + wide(two_ref, 1, block) + wide(three_ref, 0, block)
        behind = wide(one_ref, 1, block) + wide(two_ref, 0, block)
        sums = (ahead, behind, wide(one_ref, 2, block), wide(two_ref, 2, block))
        for index, (out, total) in enumerate(zip(outs, sums)):
            out[block] = (wide(kept_ref, index, block) + total).astype(out.dtype)


def combine(arrived, kept):
    outs = [jax.ShapeDtypeStruct(kept.shape[1:], kept.dtype)] * kept.shape[0]
    size = 3 * kept.size
    return call(combine_kernel, "combine_terms", outs, [None] * 4, (), size, 2 * size)(*arrived, kept)


def spread_kernel(*refs):
    own_ref, *terms, out_ref = refs
    blocks = own_ref.shape[1]
    for block in range(blocks):
        total = own_ref[0, block].astype(jnp.float32)
        for term in terms:
            total = total + term[block].astype(jnp.float32)
        total = total.astype(out_ref.dtype)
        for copy in range(SPLIT[0]):
            out_ref[copy * blocks + block] = total


def spread(own, terms):
    blocks, *inside = own.shape[1:]
    out = jax.ShapeDtypeStruct((blocks * SPLIT[0], *inside), own.dtype)
    ins = [None] * (1 + len(terms))
    size = len(ins) * own.size
    return call(spread_kernel, "spread_sum", out, ins, (), size, 2 * size)(own, *terms)


def sum_at_holder(one, two, three, kept, own):
    arrived = (mirrored(one, 1), mirrored(two, -1), mirrored(three, 2))
    sums = combine(arrived, kept)
    return spread(own, [mirrored(total, step) for total, step in zip(sums, (4, -4, 1, -1))])


def iterate_kernel(mine_ref, other_ref, out_ref, wide_ref):
    count, piece_rows, width = mine_ref.shape
    slab = count * piece_rows // SPLIT[0]
    square = jnp.zeros((piece_rows, width), jnp.float32)
    for side, ref in enumerate((mine_ref, other_ref)):
        for index in range(count):
            piece = ref[index].astype(jnp.float32)
            square = square + piece * piece
            row = (side * count + index) * piece_rows
            wide_ref[row : row + piece_rows, :] = piece
    blend = 1.0 + decay_rate
    total = jnp.sum(jnp.sum(square, axis=0, keepdims=True), axis=1, keepdims=True)
    scale = blend / (blend * jnp.sqrt(total) + norm_eps)
    wide_ref[...] = wide_ref[...] * scale

    def dot(left, right, across):
        return lax.dot_general(
            left, right, (((1,), (across,)), ((), ())), preferred_element_type=jnp.float32
        )

    narrow = lambda value: value.astype(jnp.bfloat16)
    for iteration in range(ITERS):
        last = iteration == ITERS - 1
        current = wide_ref[...]
        currents = narrow(current)
        if last:
            kept = wide_ref[pl.ds(lax.axis_index("yb") * slab, slab), :]
            mine = dot(narrow(kept), currents, 1)
            squared = narrow(dot(currents, currents, 1))
            polynomial = newton_b * mine + newton_c * dot(narrow(mine), squared, 0)
        else:
            kept = current
            mine = dot(currents, currents, 1)
            squared = narrow(mine)
            polynomial = newton_b * mine + newton_c * dot(squared, squared, 0)
        following = newton_a * kept + dot(narrow(polynomial), currents, 0)
        if not last:
            wide_ref[...] = following
    result = following * math.sqrt(width)
    for piece in range(slab // piece_rows):
        rows = result[piece * piece_rows : (piece + 1) * piece_rows, :]
        out_ref[piece] = rows.astype(out_ref.dtype)


def iterate(mine, other):
    count, piece_rows, width = mine.shape
    rows = 2 * count * piece_rows
    out = jax.ShapeDtypeStruct((count // SPLIT[0], piece_rows, width), mine.dtype)
    return call(
        iterate_kernel,
        "iterate_block",
        out,
        [None] * 2,
        [pltpu.VMEM((rows, width), jnp.float32)],
        3 * ITERS * 2 * rows * rows * width,
        4 * rows * width,
    )(mine, other)


def body(gradients, momentum, owners):
    dp_count = lax.axis_size("dp")
    my_group = lax.axis_index("dp")
    pieces = gradients[0]
    blocks_all, piece_rows, width = pieces.shape
    per_group = blocks_all // dp_count
    capacity = momentum.shape[1]
    places = jnp.arange(blocks_all, dtype=jnp.int32)
    slot_rank = ranks_of(owners)
    slot_ids = jnp.arange(capacity, dtype=jnp.int32)
    mine = owners == my_group
    grouped = pieces.reshape(dp_count, per_group, piece_rows, width)
    held = sum_at_holder(*join_momentum(grouped, momentum[0], owners))
    arrived = exchange(held, CHIPS)
    partner = lax.ppermute(arrived, "tc", [(0, 1), (1, 0)])
    back = exchange(iterate(arrived, partner), HOLD)
    groups = jnp.arange(dp_count, dtype=jnp.int32)
    held_owner = lax.dynamic_slice_in_dim(owners, my_group * per_group, per_group)
    held_rank = ranks_of(held_owner)
    held_places = jnp.arange(per_group, dtype=jnp.int32)
    pair_ids = jnp.arange(PAIR, dtype=jnp.int32)
    matched = (held_owner[:, None, None] == groups[None, :, None]) & (
        held_rank[:, None, None] == pair_ids[None, None, :]
    )
    source = jnp.sum(jnp.where(matched, held_places[:, None, None], 0), axis=0).reshape(-1)
    incoming = exchange(jnp.take(back, source, axis=0, mode="clip"), "dp")
    group_rank = ranks_of(owners * dp_count + places // per_group)
    position = places // per_group * PAIR + group_rank
    my_slots = mine[:, None] & (slot_rank[:, None] == slot_ids[None, :])
    arriving = jnp.sum(jnp.where(my_slots, position[:, None], 0), axis=0)
    occupied = jnp.any(my_slots, axis=0)
    chosen = jnp.take(incoming, arriving, axis=0, mode="clip").astype(jnp.float32)
    return jnp.where(occupied[:, None, None], chosen, 0.0)[None]


def solution(mesh):
    split = Mesh(mesh.devices.reshape(mesh.shape["dp"], *SPLIT), ("dp", *TENSOR))
    in_specs = (P("dp", None, TENSOR, None), P("dp", None, TENSOR, None), P())
    out_specs = P("dp", None, TENSOR, None)
    return jax.shard_map(body, mesh=split, in_specs=in_specs, out_specs=out_specs, check_vma=False)
```

```python
import math

import jax
import jax.numpy as jnp
from jax import lax
from jax.experimental import pallas as pl
from jax.experimental.pallas import tpu as pltpu
from jax.sharding import Mesh
from jax.sharding import PartitionSpec as P

ITERS = 3
PAIR = 3
TENSOR = ("yb", "ya", "tx", "tc")
CHIPS = ("yb", "ya", "tx")
HOLD = ("ya", "tx")
SPLIT = (2, 4, 4, 2)
VMEM_LIMIT = 12 * 1024 * 1024
PLACES = ((5, -3, 1), (-5, 3, -1), (6,), (2,), (-2,), (4, -4), (0,))


decay_rate = 0.95
newton_a = 3.4445
newton_b = -4.775
newton_c = 2.0315
norm_eps = 1e-07


def exchange(pieces, axes):
    return lax.all_to_all(pieces, axes, split_axis=0, concat_axis=0, tiled=True)


def mirrored(pieces, step):
    count, cores = lax.axis_size("dp"), lax.axis_size("tc")
    pairs = [
        (i * cores + core, (i + (step if core else -step)) % count * cores + core)
        for i in range(count)
        for core in range(cores)
    ]
    return lax.ppermute(pieces, ("dp", "tc"), pairs)


def ranks_of(labels):
    length = labels.shape[0]
    places = jnp.arange(length, dtype=jnp.int32)
    earlier = (labels[None, :] == labels[:, None]) & (places[None, :] < places[:, None])
    return jnp.sum(earlier.astype(jnp.int32), axis=1)


def call(kernel, outs, ins, scratch=(), flops=0, size=0, limit=VMEM_LIMIT):
    vmem = pl.BlockSpec(memory_space=pltpu.VMEM)
    return pl.pallas_call(
        kernel,
        out_shape=outs,
        in_specs=[vmem if space is None else pl.BlockSpec(memory_space=space) for space in ins],
        out_specs=jax.tree.map(lambda _: vmem, outs),
        scratch_shapes=list(scratch),
        cost_estimate=pl.CostEstimate(flops=flops, bytes_accessed=size, transcendentals=0),
        compiler_params=pltpu.CompilerParams(vmem_limit_bytes=limit),
    )


def join_kernel(owners_ref, pieces_ref, momentum_ref, *refs):
    *outs, held_owners, found_ref, bounds_ref, slots_ref, sems = refs
    weight = decay_rate * decay_rate / (1.0 + decay_rate)
    count, per_group = pieces_ref.shape[:2]
    me = lax.axis_index("dp")
    side = 2 * lax.axis_index("tc") - 1
    table = pltpu.make_async_copy(owners_ref, held_owners, sems.at[0])
    table.start()
    slots = pltpu.make_async_copy(momentum_ref, slots_ref, sems.at[1])
    slots.start()
    jobs = []
    for out, aways in zip(outs, PLACES):
        for index, away in enumerate(aways):
            group = lax.rem(me + away * side + count, count)
            copy = pltpu.make_async_copy(
                pieces_ref.at[group], out.at[index], sems.at[2 + len(jobs)]
            )
            jobs.append((copy, group, out.at[index]))
    for copy, _, _ in jobs:
        copy.start()
    table.wait()
    found = jnp.int32(0)
    for group in range(count):
        bounds_ref[group] = found
        for inside in range(per_group):
            found_ref[found] = inside
            found = found + (held_owners[group * per_group + inside] == me).astype(jnp.int32)
    bounds_ref[count] = found
    slots.wait()
    for copy, group, target in jobs:
        copy.wait()

        def add(slot, carry, target=target):
            inside = found_ref[slot]
            extra = weight * slots_ref[slot].astype(jnp.float32)
            target[inside] = (target[inside].astype(jnp.float32) + extra).astype(target.dtype)
            return carry

        lax.fori_loop(bounds_ref[group], bounds_ref[group + 1], add, 0)


def join_momentum(pieces, momentum, owners):
    count, *inside = pieces.shape
    outs = [jax.ShapeDtypeStruct((len(aways), *inside), pieces.dtype) for aways in PLACES]
    scratch = [
        pltpu.SMEM(owners.shape, jnp.int32),
        pltpu.SMEM((owners.shape[0] + 1,), jnp.int32),
        pltpu.SMEM((count + 1,), jnp.int32),
        pltpu.VMEM(momentum.shape, momentum.dtype),
        pltpu.SemaphoreType.DMA((2 + count,)),
    ]
    hbm = [pltpu.with_memory_space_constraint(x, pltpu.HBM) for x in (owners, pieces, momentum)]
    size = 2 * pieces.size
    return call(join_kernel, outs, [pltpu.HBM] * 3, scratch, size, 2 * size)(*hbm)


def combine_kernel(one_ref, two_ref, three_ref, kept_ref, ahead_ref, behind_ref):
    wide = lambda ref, index, block: ref[index, block].astype(jnp.float32)
    for block in range(kept_ref.shape[1]):
        ahead = wide(one_ref, 0, block) + wide(two_ref, 1, block) + wide(three_ref, 0, block)
        behind = wide(one_ref, 1, block) + wide(two_ref, 0, block)
        ahead_ref[block] = (wide(kept_ref, 0, block) + ahead).astype(ahead_ref.dtype)
        behind_ref[block] = (wide(kept_ref, 1, block) + behind).astype(behind_ref.dtype)


def combine(arrived, kept):
    outs = [jax.ShapeDtypeStruct(kept.shape[1:], kept.dtype)] * kept.shape[0]
    size = 4 * kept.size
    return call(combine_kernel, outs, [None] * 4, (), size, 2 * size)(*arrived, kept)


def spread_kernel(*refs):
    *terms, out_ref = refs
    blocks = terms[0].shape[1]
    for block in range(blocks):
        total = terms[0][terms[0].shape[0] - 1, block].astype(jnp.float32)
        for term in terms[1:]:
            total = total + term[term.shape[0] - 1, block].astype(jnp.float32)
        total = total.astype(out_ref.dtype)
        for copy in range(SPLIT[0]):
            out_ref[copy * blocks + block] = total


def spread(terms):
    blocks, *inside = terms[0].shape[1:]
    out = jax.ShapeDtypeStruct((blocks * SPLIT[0], *inside), terms[0].dtype)
    size = len(terms) * blocks * math.prod(inside)
    return call(spread_kernel, out, [None] * len(terms), (), size, 2 * size)(*terms)


def sum_at_holder(one, two, three, four, five, kept, own):
    corner = mirrored(three, 2)
    arrived = (mirrored(one, 1), mirrored(two, -1), corner)
    direct = [mirrored(four, 2), mirrored(five, -2)]
    sums = [mirrored(total, step)[None] for total, step in zip(combine(arrived, kept), (4, -4))]
    return spread([own, *arrived[:2], *direct, *sums])


def iterate_kernel(mine_ref, other_ref, out_ref, wide_ref):
    count, piece_rows, width = mine_ref.shape
    slab = count * piece_rows // SPLIT[0]
    square = jnp.zeros((piece_rows, width), jnp.float32)
    for side, ref in enumerate((mine_ref, other_ref)):
        for index in range(count):
            piece = ref[index].astype(jnp.float32)
            square = square + piece * piece
            row = (side * count + index) * piece_rows
            wide_ref[row : row + piece_rows, :] = piece
    blend = 1.0 + decay_rate
    total = jnp.sum(jnp.sum(square, axis=0, keepdims=True), axis=1, keepdims=True)
    scale = blend / (blend * jnp.sqrt(total) + norm_eps)
    wide_ref[...] = wide_ref[...] * scale

    def dot(left, right, across):
        return lax.dot_general(
            left, right, (((1,), (across,)), ((), ())), preferred_element_type=jnp.float32
        )

    narrow = lambda value: value.astype(jnp.bfloat16)
    for iteration in range(ITERS):
        last = iteration == ITERS - 1
        current = wide_ref[...]
        currents = narrow(current)
        if last:
            kept = wide_ref[pl.ds(lax.axis_index("yb") * slab, slab), :]
            mine = dot(narrow(kept), currents, 1)
            squared = narrow(dot(currents, currents, 1))
            polynomial = newton_b * mine + newton_c * dot(narrow(mine), squared, 0)
        else:
            kept = current
            mine = dot(currents, currents, 1)
            squared = narrow(mine)
            polynomial = newton_b * mine + newton_c * dot(squared, squared, 0)
        following = newton_a * kept + dot(narrow(polynomial), currents, 0)
        if not last:
            wide_ref[...] = following
    result = following * math.sqrt(width)
    for piece in range(slab // piece_rows):
        rows = result[piece * piece_rows : (piece + 1) * piece_rows, :]
        out_ref[piece] = rows.astype(out_ref.dtype)


def iterate(mine, other):
    count, piece_rows, width = mine.shape
    rows = 2 * count * piece_rows
    out = jax.ShapeDtypeStruct((count // SPLIT[0], piece_rows, width), mine.dtype)
    return call(
        iterate_kernel,
        out,
        [None] * 2,
        [pltpu.VMEM((rows, width), jnp.float32)],
        3 * ITERS * 2 * rows * rows * width,
        4 * rows * width,
    )(mine, other)


def body(gradients, momentum, owners):
    dp_count = lax.axis_size("dp")
    my_group = lax.axis_index("dp")
    pieces = gradients[0]
    blocks_all, piece_rows, width = pieces.shape
    per_group = blocks_all // dp_count
    capacity = momentum.shape[1]
    places = jnp.arange(blocks_all, dtype=jnp.int32)
    slot_rank = ranks_of(owners)
    slot_ids = jnp.arange(capacity, dtype=jnp.int32)
    mine = owners == my_group
    grouped = pieces.reshape(dp_count, per_group, piece_rows, width)
    held = sum_at_holder(*join_momentum(grouped, momentum[0], owners))
    arrived = exchange(held, CHIPS)
    partner = lax.ppermute(arrived, "tc", [(0, 1), (1, 0)])
    back = exchange(iterate(arrived, partner), HOLD)
    groups = jnp.arange(dp_count, dtype=jnp.int32)
    held_owner = lax.dynamic_slice_in_dim(owners, my_group * per_group, per_group)
    held_rank = ranks_of(held_owner)
    held_places = jnp.arange(per_group, dtype=jnp.int32)
    pair_ids = jnp.arange(PAIR, dtype=jnp.int32)
    matched = (held_owner[:, None, None] == groups[None, :, None]) & (
        held_rank[:, None, None] == pair_ids[None, None, :]
    )
    source = jnp.sum(jnp.where(matched, held_places[:, None, None], 0), axis=0).reshape(-1)
    incoming = exchange(jnp.take(back, source, axis=0, mode="clip"), "dp")
    group_rank = ranks_of(owners * dp_count + places // per_group)
    position = places // per_group * PAIR + group_rank
    my_slots = mine[:, None] & (slot_rank[:, None] == slot_ids[None, :])
    arriving = jnp.sum(jnp.where(my_slots, position[:, None], 0), axis=0)
    occupied = jnp.any(my_slots, axis=0)
    chosen = jnp.take(incoming, arriving, axis=0, mode="clip").astype(jnp.float32)
    return jnp.where(occupied[:, None, None], chosen, 0.0)[None]


def solution(mesh):
    split = Mesh(mesh.devices.reshape(mesh.shape["dp"], *SPLIT), ("dp", *TENSOR))
    in_specs = (P("dp", None, TENSOR, None), P("dp", None, TENSOR, None), P())
    out_specs = P("dp", None, TENSOR, None)
    return jax.shard_map(body, mesh=split, in_specs=in_specs, out_specs=out_specs, check_vma=False)
```

```python
import math

import jax
import jax.numpy as jnp
from jax import lax
from jax.experimental import pallas as pl
from jax.experimental.pallas import tpu as pltpu
from jax.sharding import Mesh
from jax.sharding import PartitionSpec as P

ITERS = 3
PAIR = 3
TENSOR = ("yb", "ya", "tx", "tc")
CHIPS = ("yb", "ya", "tx")
HOLD = ("ya", "tx")
SPLIT = (2, 4, 4, 2)
VMEM_LIMIT = 12 * 1024 * 1024
PLACES = ((5, -3, 2), (-5, 3, -2), (6,), (4, -4, 1, -1), (0,))


decay_rate = 0.95
newton_a = 3.4445
newton_b = -4.775
newton_c = 2.0315
norm_eps = 1e-07


def exchange(pieces, axes):
    return lax.all_to_all(pieces, axes, split_axis=0, concat_axis=0, tiled=True)


def mirrored(pieces, step):
    count, cores = lax.axis_size("dp"), lax.axis_size("tc")
    pairs = [
        (i * cores + core, (i + (step if core else -step)) % count * cores + core)
        for i in range(count)
        for core in range(cores)
    ]
    return lax.ppermute(pieces, ("dp", "tc"), pairs)


def ranks_of(labels):
    length = labels.shape[0]
    places = jnp.arange(length, dtype=jnp.int32)
    earlier = (labels[None, :] == labels[:, None]) & (places[None, :] < places[:, None])
    return jnp.sum(earlier.astype(jnp.int32), axis=1)


def call(kernel, outs, ins, scratch=(), flops=0, size=0, limit=VMEM_LIMIT):
    vmem = pl.BlockSpec(memory_space=pltpu.VMEM)
    return pl.pallas_call(
        kernel,
        out_shape=outs,
        in_specs=[vmem if space is None else pl.BlockSpec(memory_space=space) for space in ins],
        out_specs=jax.tree.map(lambda _: vmem, outs),
        scratch_shapes=list(scratch),
        cost_estimate=pl.CostEstimate(flops=flops, bytes_accessed=size, transcendentals=0),
        compiler_params=pltpu.CompilerParams(vmem_limit_bytes=limit),
    )


def join_kernel(owners_ref, pieces_ref, momentum_ref, *refs):
    *outs, held_owners, found_ref, bounds_ref, slots_ref, sems = refs
    weight = decay_rate * decay_rate / (1.0 + decay_rate)
    count, per_group = pieces_ref.shape[:2]
    me = lax.axis_index("dp")
    side = 2 * lax.axis_index("tc") - 1
    table = pltpu.make_async_copy(owners_ref, held_owners, sems.at[0])
    table.start()
    slots = pltpu.make_async_copy(momentum_ref, slots_ref, sems.at[1])
    slots.start()
    jobs = []
    for out, aways in zip(outs, PLACES):
        for index, away in enumerate(aways):
            group = lax.rem(me + away * side + count, count)
            copy = pltpu.make_async_copy(
                pieces_ref.at[group], out.at[index], sems.at[2 + len(jobs)]
            )
            jobs.append((copy, group, out.at[index]))
    for copy, _, _ in jobs:
        copy.start()
    table.wait()
    found = jnp.int32(0)
    for group in range(count):
        bounds_ref[group] = found
        for inside in range(per_group):
            found_ref[found] = inside
            found = found + (held_owners[group * per_group + inside] == me).astype(jnp.int32)
    bounds_ref[count] = found
    slots.wait()
    for copy, group, target in jobs:
        copy.wait()

        def add(slot, carry, target=target):
            inside = found_ref[slot]
            extra = weight * slots_ref[slot].astype(jnp.float32)
            target[inside] = (target[inside].astype(jnp.float32) + extra).astype(target.dtype)
            return carry

        lax.fori_loop(bounds_ref[group], bounds_ref[group + 1], add, 0)


def join_momentum(pieces, momentum, owners):
    count, *inside = pieces.shape
    outs = [jax.ShapeDtypeStruct((len(aways), *inside), pieces.dtype) for aways in PLACES]
    scratch = [
        pltpu.SMEM(owners.shape, jnp.int32),
        pltpu.SMEM((owners.shape[0] + 1,), jnp.int32),
        pltpu.SMEM((count + 1,), jnp.int32),
        pltpu.VMEM(momentum.shape, momentum.dtype),
        pltpu.SemaphoreType.DMA((2 + count,)),
    ]
    hbm = [pltpu.with_memory_space_constraint(x, pltpu.HBM) for x in (owners, pieces, momentum)]
    size = 2 * pieces.size
    return call(join_kernel, outs, [pltpu.HBM] * 3, scratch, size, 2 * size)(*hbm)


def near_kernel(one_ref, kept_ref, out_ref):
    for block in range(out_ref.shape[0]):
        total = kept_ref[2, block].astype(jnp.float32) + one_ref[2, block].astype(jnp.float32)
        out_ref[block] = total.astype(out_ref.dtype)


def combine_kernel(one_ref, two_ref, three_ref, kept_ref, *outs):
    wide = lambda ref, index, block: ref[index, block].astype(jnp.float32)
    for block in range(kept_ref.shape[1]):
        ahead = wide(one_ref, 0, block) + wide(two_ref, 1, block) + wide(three_ref, 0, block)
        behind = wide(one_ref, 1, block) + wide(two_ref, 0, block)
        sums = (ahead, behind, wide(two_ref, 2, block))
        for kept, out, total in zip((0, 1, 3), outs, sums):
            out[block] = (wide(kept_ref, kept, block) + total).astype(out.dtype)


def combine(kernel, count, *terms):
    outs = [jax.ShapeDtypeStruct(terms[0].shape[1:], terms[0].dtype)] * count
    size = 3 * count * math.prod(outs[0].shape)
    ins = [None] * len(terms)
    return call(kernel, outs, ins, (), size, 2 * size)(*terms)


def spread_kernel(*refs):
    own_ref, *terms, out_ref = refs
    blocks = own_ref.shape[1]
    for block in range(blocks):
        total = own_ref[0, block].astype(jnp.float32)
        for term in terms:
            total = total + term[block].astype(jnp.float32)
        total = total.astype(out_ref.dtype)
        for copy in range(SPLIT[0]):
            out_ref[copy * blocks + block] = total


def spread(own, terms):
    blocks, *inside = own.shape[1:]
    out = jax.ShapeDtypeStruct((blocks * SPLIT[0], *inside), own.dtype)
    ins = [None] * (1 + len(terms))
    size = len(ins) * own.size
    return call(spread_kernel, out, ins, (), size, 2 * size)(own, *terms)


def sum_at_holder(one, two, three, kept, own):
    three = mirrored(three, 2)
    one = mirrored(one, 1)
    two = mirrored(two, -1)
    (near,) = combine(near_kernel, 1, one, kept)
    near = mirrored(near, 1)
    sums = combine(combine_kernel, 3, one, two, three, kept)
    return spread(own, [near, *(mirrored(total, step) for total, step in zip(sums, (4, -4, -1)))])


def iterate_kernel(mine_ref, other_ref, out_ref, wide_ref):
    count, piece_rows, width = mine_ref.shape
    slab = count * piece_rows // SPLIT[0]
    square = jnp.zeros((piece_rows, width), jnp.float32)
    for side, ref in enumerate((mine_ref, other_ref)):
        for index in range(count):
            piece = ref[index].astype(jnp.float32)
            square = square + piece * piece
            row = (side * count + index) * piece_rows
            wide_ref[row : row + piece_rows, :] = piece
    blend = 1.0 + decay_rate
    total = jnp.sum(jnp.sum(square, axis=0, keepdims=True), axis=1, keepdims=True)
    scale = blend / (blend * jnp.sqrt(total) + norm_eps)
    wide_ref[...] = wide_ref[...] * scale

    def dot(left, right, across):
        return lax.dot_general(
            left, right, (((1,), (across,)), ((), ())), preferred_element_type=jnp.float32
        )

    narrow = lambda value: value.astype(jnp.bfloat16)
    for iteration in range(ITERS):
        last = iteration == ITERS - 1
        current = wide_ref[...]
        currents = narrow(current)
        if last:
            kept = wide_ref[pl.ds(lax.axis_index("yb") * slab, slab), :]
            mine = dot(narrow(kept), currents, 1)
            squared = narrow(dot(currents, currents, 1))
            polynomial = newton_b * mine + newton_c * dot(narrow(mine), squared, 0)
        else:
            kept = current
            mine = dot(currents, currents, 1)
            squared = narrow(mine)
            polynomial = newton_b * mine + newton_c * dot(squared, squared, 0)
        following = newton_a * kept + dot(narrow(polynomial), currents, 0)
        if not last:
            wide_ref[...] = following
    result = following * math.sqrt(width)
    for piece in range(slab // piece_rows):
        rows = result[piece * piece_rows : (piece + 1) * piece_rows, :]
        out_ref[piece] = rows.astype(out_ref.dtype)


def iterate(mine, other):
    count, piece_rows, width = mine.shape
    rows = 2 * count * piece_rows
    out = jax.ShapeDtypeStruct((count // SPLIT[0], piece_rows, width), mine.dtype)
    return call(
        iterate_kernel,
        out,
        [None] * 2,
        [pltpu.VMEM((rows, width), jnp.float32)],
        3 * ITERS * 2 * rows * rows * width,
        4 * rows * width,
    )(mine, other)


def body(gradients, momentum, owners):
    dp_count = lax.axis_size("dp")
    my_group = lax.axis_index("dp")
    pieces = gradients[0]
    blocks_all, piece_rows, width = pieces.shape
    per_group = blocks_all // dp_count
    capacity = momentum.shape[1]
    places = jnp.arange(blocks_all, dtype=jnp.int32)
    slot_rank = ranks_of(owners)
    slot_ids = jnp.arange(capacity, dtype=jnp.int32)
    mine = owners == my_group
    grouped = pieces.reshape(dp_count, per_group, piece_rows, width)
    held = sum_at_holder(*join_momentum(grouped, momentum[0], owners))
    arrived = exchange(held, CHIPS)
    partner = lax.ppermute(arrived, "tc", [(0, 1), (1, 0)])
    back = exchange(iterate(arrived, partner), HOLD)
    groups = jnp.arange(dp_count, dtype=jnp.int32)
    held_owner = lax.dynamic_slice_in_dim(owners, my_group * per_group, per_group)
    held_rank = ranks_of(held_owner)
    held_places = jnp.arange(per_group, dtype=jnp.int32)
    pair_ids = jnp.arange(PAIR, dtype=jnp.int32)
    matched = (held_owner[:, None, None] == groups[None, :, None]) & (
        held_rank[:, None, None] == pair_ids[None, None, :]
    )
    source = jnp.sum(jnp.where(matched, held_places[:, None, None], 0), axis=0).reshape(-1)
    incoming = exchange(jnp.take(back, source, axis=0, mode="clip"), "dp")
    group_rank = ranks_of(owners * dp_count + places // per_group)
    position = places // per_group * PAIR + group_rank
    my_slots = mine[:, None] & (slot_rank[:, None] == slot_ids[None, :])
    arriving = jnp.sum(jnp.where(my_slots, position[:, None], 0), axis=0)
    occupied = jnp.any(my_slots, axis=0)
    chosen = jnp.take(incoming, arriving, axis=0, mode="clip").astype(jnp.float32)
    return jnp.where(occupied[:, None, None], chosen, 0.0)[None]


def solution(mesh):
    split = Mesh(mesh.devices.reshape(mesh.shape["dp"], *SPLIT), ("dp", *TENSOR))
    in_specs = (P("dp", None, TENSOR, None), P("dp", None, TENSOR, None), P())
    out_specs = P("dp", None, TENSOR, None)
    return jax.shard_map(body, mesh=split, in_specs=in_specs, out_specs=out_specs, check_vma=False)
```
